32 devices in a mesh: groups: 2 (over x), rows: 16 (over z, y, core).
Axes of the slice: x: 2, y: 2, z: 4, core: 2. Of those that a mesh axis runs over, the one named last changes fastest.
Arguments:
- frames: bfloat16 [16384, 2560], P(('groups', 'rows')), parts along dimension 0, may hold values from -6 to 6
- offsets: int32 [4096], P(('groups', 'rows')), parts along dimension 0, may hold values from 0 to 8173, as said below
- neighbours: int32 [32, 4096], P(None, ('groups', 'rows')), parts along dimension 1, may hold values from 0 to 2047, as said below
- initial_codes: int32 [32, 4096], P(None, ('groups', 'rows')), parts along dimension 1, may hold values from -1048576 to 1048575
- embed_weight: bfloat16 [2560, 256], replicated, may hold values from -0.125 to 0.125
- embed_bias: float32 [256], replicated, may hold values from -0.9 to 0.9
Outputs:
- affinity: float32 [32, 4096], P(None, ('groups', 'rows')), parts along dimension 1
- vectors: float32 [32, 4096], P(None, ('groups', 'rows')), parts along dimension 1
The draws below stay inside these ranges and needn't reach their ends.
There are 2 independent parts, one for each index of `groups`. The reference program is written for one: setup_inputs(seed, part) draws one part's arguments, and reference() takes and returns one part's arrays. A program takes and returns all parts, laid end to end along the dimension named above; an argument that names none is the same for every part. Nothing has to cross between parts.
Inputs may be any that keep to these rules, and one draw needn't show every extreme that they name: `offsets`: the window of row i starts in the block of 512 frames numbered i // 128 and its 19 frames end before frame 8192. `neighbours`: the 32 columns of row i are distinct and differ from i; the k-th is (i + d) mod 2048 with 1 + k s <= d <= (k + 1) s, where s = 63.
All inputs are finite; a program needn't handle non-finite values.
Results may differ from the reference program's by a relative error of at most 0.012.
The reference program's roundings to bfloat16 on the way (of `pooled` and `unit_rows`) count: a program that leaves them out, or rounds other values in their place, can miss the bound.
Values may be sent and summed in bfloat16 or wider, within the bound.
No kernel may reach another device: no remote copies, remote signals or barrier semaphores. Data moves between devices by JAX's collectives and lax.ppermute only.
A program may use at most 64 MiB of HBM per device.

```python
from functools import partial
import jax
import jax.numpy as jnp
from jax import lax

C = 2560
EMB = 256
WIN = 19
K = 32
V = 32
ITERS = 3
ROWS_DEV = 128
FR_DEV = 512
N = 2048
NFR = 8192


def draw_offsets(key, part):
    row_ids = jnp.arange(N, dtype=jnp.int32)
    device = row_ids // ROWS_DEV
    inside = row_ids % ROWS_DEV
    inner_key = jax.random.fold_in(key, 11)
    rim_key = jax.random.fold_in(key, 12)
    spread = jax.random.randint(inner_key, (N,), 0, FR_DEV - WIN + 1, dtype=jnp.int32)
    rim_pick = jax.random.randint(rim_key, (N,), 0, WIN - 1, dtype=jnp.int32)
    crossing = (inside == ROWS_DEV - 1) & (device < N // ROWS_DEV - 1)
    local_start = jnp.where(crossing, FR_DEV - 1 - rim_pick, spread)
    return device * FR_DEV + local_start


def draw_neighbours(key, part):
    stride = (N - 1) // K
    jitter = jax.random.randint(jax.random.fold_in(key, 21), (K, N), 0, stride, dtype=jnp.int32)
    band = jnp.arange(K, dtype=jnp.int32)[:, None] * stride
    row_ids = jnp.arange(N, dtype=jnp.int32)[None, :]
    return (row_ids + 1 + band + jitter) % N


def with_ends(entries, stream_key, least, largest):
    spot = [jax.random.randint(jax.random.fold_in(stream_key, axis), (), 0, length) for axis, length in enumerate(entries.shape)]
    main_axis = entries.shape.index(max(entries.shape))
    next_to = spot[:main_axis] + [(spot[main_axis] + 1) % entries.shape[main_axis]] + spot[main_axis + 1:]
    return entries.at[tuple(spot)].set(least).at[tuple(next_to)].set(largest)


def block_levels(stream_key, dims, shards, least, top_value):
    def one(position, parts):
        draws = jax.random.uniform(jax.random.fold_in(jax.random.fold_in(stream_key, 6), position), (parts,), jnp.float32, least / len(shards), top_value / len(shards))
        return jnp.repeat(jnp.exp(draws), dims[position] // parts).reshape((-1,) + (1,) * (len(dims) - position - 1))

    gain = one(*shards[0])
    for cut in shards[1:]:
        gain = gain * one(*cut)
    return gain


def gaussian(own_key, shape, deviation, limit, cuts=(), kind=jnp.bfloat16):
    drawn = deviation * jax.random.normal(own_key, shape, jnp.float32)
    if cuts:
        drawn = drawn * block_levels(own_key, shape, cuts, -0.22, 0.18)
    return jnp.clip(drawn, -limit, limit).astype(kind)


def setup_inputs(seed: int = 0, part: int = 0) -> dict:
    keys = jax.random.split(jax.random.key(seed), 7)
    own_keys = jax.random.split(jax.random.fold_in(keys[6], part), 7)
    frames = gaussian(own_keys[0], (NFR, C), 1.0, 6.0, ((0, 16),))
    offsets = draw_offsets(jax.random.fold_in(jax.random.fold_in(keys[6], part), 71), part)
    neighbours = draw_neighbours(jax.random.fold_in(jax.random.fold_in(keys[6], part), 71), part)
    initial_codes = with_ends(jax.random.randint(own_keys[3], (V, N), -1048576, 1048576), jax.random.fold_in(own_keys[3], 1), -1048576, 1048575).astype(jnp.int32)
    embed_weight = gaussian(keys[4], (C, EMB), C ** -0.5, 0.125)
    embed_bias = gaussian(keys[5], (EMB,), 0.15, 0.9, (), jnp.float32)
    return dict(frames=frames, offsets=offsets, neighbours=neighbours, initial_codes=initial_codes, embed_weight=embed_weight, embed_bias=embed_bias)


epsilon = 1e-06
sharpness = 8.0
seed_scale = 2.0 ** (-20)

def pool_block(frames, block_offsets):

    def one_window(anchor):
        return lax.dynamic_slice_in_dim(frames, anchor, WIN, 0)
    windows = jax.vmap(one_window)(block_offsets)
    return (lax.optimization_barrier(jnp.sum(windows.astype(jnp.float32), axis=1)) * (1.0 / WIN)).astype(jnp.bfloat16)

def reference(frames, offsets, neighbours, initial_codes, embed_weight, embed_bias):
    pooled = lax.map(partial(pool_block, frames), offsets.reshape(-1, ROWS_DEV)).reshape(N, C)
    embedded = jnp.dot(pooled.astype(jnp.float32), embed_weight.astype(jnp.float32), preferred_element_type=jnp.float32) + embed_bias
    squares = lax.optimization_barrier(jnp.sum(embedded * embedded, axis=1, keepdims=True))
    unit_rows = (embedded * lax.rsqrt(squares + epsilon)).astype(jnp.bfloat16)
    columns = neighbours.T.reshape(-1, ROWS_DEV, K)

    def cosine_block(packed):
        rows_block, cols_block = packed
        neighbour_rows = jnp.take(unit_rows, cols_block, axis=0)
        return jnp.einsum('be,bke->bk', rows_block.astype(jnp.float32), neighbour_rows.astype(jnp.float32), precision=lax.Precision.HIGHEST)
    cosine = lax.map(cosine_block, (unit_rows.reshape(-1, ROWS_DEV, EMB), columns)).reshape(N, K).T
    affinity = jnp.exp(sharpness * (cosine - 1.0))
    vectors = initial_codes.astype(jnp.float32) * seed_scale
    for turn_index in range(ITERS):
        forward = lax.optimization_barrier(jnp.sum(affinity[None] * jnp.take(vectors, neighbours, axis=1), axis=1))
        backward = jnp.zeros_like(vectors).at[:, neighbours.reshape(-1)].add((affinity[None] * vectors[:, None, :]).reshape(vectors.shape[0], -1))
        mixed = 0.5 * (forward + backward)
        gram_matrix = jnp.dot(mixed, mixed.T, precision=lax.Precision.HIGHEST)
        cholesky_factor = jnp.linalg.cholesky(gram_matrix)
        vectors = jax.scipy.linalg.solve_triangular(cholesky_factor, mixed, lower=True)
    return (affinity, vectors)
```

```python
import functools
import math

import jax
import jax.numpy as jnp
from jax import lax
from jax.experimental import pallas as pl
from jax.experimental.pallas import tpu as pltpu
from jax.sharding import PartitionSpec as P

WIN = 19
ITERS = 3


epsilon = 1e-06
sharpness = 8.0
seed_scale = 2.0 ** (-20)


def from_behind(block, axis, distance):
    devices = range(lax.axis_size(axis))
    route = [(i - distance, i) for i in devices if i - distance in devices]
    return lax.ppermute(block, axis, route)


def block_width(length, shard_rows):
    shards = length // shard_rows
    chosen = 1
    for factor in range(1, shards + 1):
        if shards % factor == 0 and factor * shard_rows <= 4096:
            chosen = factor
    return chosen * shard_rows


def on_device_sharded(frames, offsets, neighbours, initial_codes, embed_weight, embed_bias):
    own_rows = offsets.shape[0]
    own_frames = frames.shape[0]
    kept = neighbours.shape[0]
    my_index = lax.axis_index("rows")
    next_frames = from_behind(frames[: WIN - 1], "rows", -1)
    extended = jnp.concatenate([frames, next_frames], axis=0)
    window_start = offsets - my_index * own_frames
    positions = jnp.arange(extended.shape[0], dtype=jnp.int32)[None, :]
    begins = window_start[:, None]
    window_mask = ((positions >= begins) & (positions < begins + WIN)).astype(jnp.bfloat16)
    window_sums = jnp.dot(window_mask, extended, preferred_element_type=jnp.float32)
    pooled = (window_sums * (1.0 / WIN)).astype(jnp.bfloat16)
    embedded = jnp.dot(pooled, embed_weight, preferred_element_type=jnp.float32) + embed_bias
    squares = jnp.sum(embedded * embedded, axis=1, keepdims=True)
    unit_rows = (embedded * lax.rsqrt(squares + epsilon)).astype(jnp.bfloat16)
    portion = lax.all_gather(unit_rows, "rows", axis=0, tiled=True)
    length = portion.shape[0]
    block_cols = block_width(length, own_rows)

    def one_block(block_index, carried):
        first_col = block_index * block_cols
        candidates = lax.dynamic_slice_in_dim(portion, first_col, block_cols, 0)
        scores = lax.dot_general(
            unit_rows, candidates, (((1,), (1,)), ((), ())), preferred_element_type=jnp.float32
        )
        relative = neighbours - first_col
        inside = (relative >= 0) & (relative < block_cols)
        picked = jnp.take_along_axis(scores, jnp.clip(relative, 0, block_cols - 1).T, axis=1).T
        return carried + jnp.where(inside, picked, 0.0)

    cosine = lax.fori_loop(
        0, length // block_cols, one_block, jnp.zeros((kept, own_rows), jnp.float32)
    )
    affinity = jnp.exp(sharpness * (cosine - 1.0))
    vectors = initial_codes.astype(jnp.float32) * seed_scale
    vec_count = vectors.shape[0]
    carried = vectors
    for turn_index in range(ITERS):
        gathered = lax.all_gather(carried, "rows", axis=1, tiled=True)
        if turn_index > 0:
            gram_matrix = jnp.dot(gathered, gathered.T, precision=lax.Precision.HIGHEST)
            cholesky_factor = jnp.linalg.cholesky(gram_matrix)
            gathered = jax.scipy.linalg.solve_triangular(cholesky_factor, gathered, lower=True)
        current = lax.dynamic_slice_in_dim(gathered, my_index * own_rows, own_rows, 1)
        forward = jnp.sum(affinity[None] * jnp.take(gathered, neighbours, axis=1), axis=1)
        spread = (
            jnp.zeros((vec_count, gathered.shape[1]), jnp.float32)
            .at[:, neighbours.reshape(-1)]
            .add((affinity[None] * current[:, None, :]).reshape(vec_count, -1))
        )
        mixed = 0.5 * (forward + lax.psum_scatter(spread, "rows", scatter_dimension=1, tiled=True))
        carried = mixed
    partial_gram = jnp.dot(carried, carried.T, precision=lax.Precision.HIGHEST)
    gram_matrix = lax.psum(partial_gram, "rows")
    cholesky_factor = jnp.linalg.cholesky(gram_matrix)
    carried = jax.scipy.linalg.solve_triangular(cholesky_factor, carried, lower=True)
    return (affinity, carried)


BF = jnp.bfloat16
F32 = jnp.float32
DENSE_BYTES = 32 * 1024 * 1024
NT = (((1,), (1,)), ((), ()))


def split2(x):
    high = x.astype(BF)
    return high, (x - high.astype(F32)).astype(BF)


def gather_stages(own, count):
    far = count // 4
    me = lax.axis_index("rows")
    hop = lambda block, route: lax.ppermute(block, "rows", route)
    along = [own]
    for step in range(1, far):
        along.append(hop(own, [(i, (i + 4 * step) % count) for i in range(count)]))
    line = jnp.stack(along)
    pair = jnp.concatenate([line, hop(line, [(i, i ^ 2) for i in range(count)])])
    whole = jnp.concatenate([pair, hop(pair, [(i, i ^ 1) for i in range(count)])])
    owners = jnp.stack(
        [
            lax.bitwise_xor(lax.rem(me + count - 4 * step, count), flip)
            for flip in (0, 2, 1, 3)
            for step in range(far)
        ]
    )
    return whole, owners


def orthonormal_factor(gram):
    size = gram.shape[0]
    rows = lax.broadcasted_iota(jnp.int32, (size, size), 0)
    cols = lax.broadcasted_iota(jnp.int32, (size, size), 1)
    work = jnp.concatenate([gram, (rows == cols).astype(F32)], axis=1)
    row_ids = lax.broadcasted_iota(jnp.int32, (size, 1), 0)
    for k in range(size - 1):
        pivot_row = work[k : k + 1, :]
        factor = jnp.where(row_ids > k, work[:, k : k + 1] / work[k : k + 1, k : k + 1], 0.0)
        work = work - factor * pivot_row
    pivots = jnp.sum(jnp.where(rows == cols, work[:, :size], 0.0), axis=1, keepdims=True)
    return work[:, size:] * lax.rsqrt(pivots)


def dense_kernel(tile, shards, own_rows, width, kept, vec_count, col_tile_ref, near_ref, got_ref,
                 aff_ref, vec_ref, unit, codes, spots, high, low, start):
    length = shards * own_rows
    half = kept
    for s in range(shards):
        span = pl.ds(s * own_rows, own_rows)
        unit[span, :] = got_ref[s, :own_rows, :]
        extra = got_ref[s, own_rows:, :].astype(F32)
        even = extra[:half, :own_rows]
        odd = extra[half : 2 * half, :own_rows]
        product = even * odd
        upper = jnp.floor(product * (1.0 / 256.0))
        codes[pl.ds(0, half), span] = even
        codes[pl.ds(half, half), span] = odd
        codes[pl.ds(2 * half, half), span] = upper
        codes[pl.ds(3 * half, half), span] = product - 256.0 * upper
        start[:, span] = (
            extra[:vec_count, own_rows:] + extra[vec_count : 2 * vec_count, own_rows:]
        )
    col = lax.broadcasted_iota(jnp.int32, (1, length), 1)
    place = lax.rem(col, tile).astype(F32)
    tile_ids = lax.broadcasted_iota(jnp.int32, (half, length), 0)
    member = (tile_ids == col_tile_ref[...]).astype(F32)
    spots[pl.ds(0, half), :] = -place * member
    spots[pl.ds(half, half), :] = -place * member
    spots[pl.ds(2 * half, half), :] = 256.0 * member
    spots[pl.ds(3 * half, half), :] = member

    gain = sharpness / math.log(2.0)
    chunk = 512

    @pl.loop(0, shards)
    def _(b):
        span = pl.ds(pl.multiple_of(b * own_rows, own_rows), own_rows)
        my_unit = unit[span, :]
        my_codes = codes[:, span].T.astype(BF)
        my_spots = spots[:, span].T.astype(BF)
        my_place = lax.rem(lax.broadcasted_iota(jnp.int32, (own_rows, 1), 0), tile).astype(F32)
        for c in range(length // chunk):
            cols = pl.ds(c * chunk, chunk)
            scores = lax.dot_general(my_unit, unit[cols, :], NT, preferred_element_type=F32)
            ahead = jnp.dot(my_codes, spots[:, cols].astype(BF), preferred_element_type=F32)
            behind = jnp.dot(my_spots, codes[:, cols].astype(BF), preferred_element_type=F32)
            here = place[:, c * chunk : (c + 1) * chunk]
            share = jnp.where(ahead == -here * here, 0.5, 0.0) + jnp.where(
                behind == -my_place * my_place, 0.5, 0.0
            )
            weight = jnp.exp2(scores * gain - gain) * share
            top, rest = split2(weight)
            high[span, cols] = top
            low[span, cols] = rest

    own = pl.ds(0, own_rows)
    spread = member.astype(BF)
    scores = lax.dot_general(unit[own, :], unit[...], NT, preferred_element_type=F32)
    weight = jnp.exp2(scores * gain - gain)
    found = []
    for parity in range(2):
        code = codes[pl.ds(parity * half, half), own].T.astype(BF)
        mask = jnp.dot(code, spread, preferred_element_type=F32) == place
        value = jnp.where(mask, weight, 0.0)
        top, rest = split2(value)
        found.append(
            lax.dot_general(spread, top, NT, preferred_element_type=F32)
            + lax.dot_general(spread, rest, NT, preferred_element_type=F32)
        )
    near = near_ref[...]
    odd_row = lax.rem(lax.broadcasted_iota(jnp.int32, near.shape, 0), 2) == 1
    result = jnp.zeros(near.shape, F32)
    for t in range(half):
        pick = jnp.where(odd_row, found[1][t : t + 1, :], found[0][t : t + 1, :])
        result = result + jnp.where(near == t, pick, 0.0)
    aff_ref[...] = result

    current = start[...] * seed_scale
    for turn in range(ITERS):
        top, rest = split2(current)
        both = jnp.concatenate([top, rest], axis=0)
        first = jnp.dot(both, high[...], preferred_element_type=F32)
        second = jnp.dot(top, low[...], preferred_element_type=F32)
        mixed = first[:vec_count] + first[vec_count:] + second
        gram = lax.dot_general(
            mixed, mixed, NT, preferred_element_type=F32, precision=lax.Precision.HIGHEST
        )
        factor = orthonormal_factor(gram)
        if turn == ITERS - 1:
            mixed = mixed[:, :own_rows]
        current = jnp.dot(
            factor, mixed, preferred_element_type=F32, precision=lax.Precision.HIGHEST
        )
    vec_ref[...] = current


def on_device_dense(frames, offsets, neighbours, initial_codes, embed_weight, embed_bias):
    own_rows = offsets.shape[0]
    own_frames = frames.shape[0]
    kept = neighbours.shape[0]
    vec_count = initial_codes.shape[0]
    shards = lax.axis_size("rows")
    length = own_rows * shards
    tile = length // kept
    width = embed_weight.shape[1]
    my_index = lax.axis_index("rows")
    next_frames = from_behind(frames[: WIN - 1], "rows", -1)
    begins = (offsets - my_index * own_frames)[:, None]

    def window_mask(first, count):
        positions = first + jnp.arange(count, dtype=jnp.int32)[None, :]
        return ((positions >= begins) & (positions < begins + WIN)).astype(BF)

    window_sums = jnp.dot(
        window_mask(0, own_frames), frames, preferred_element_type=F32
    ) + jnp.dot(
        window_mask(own_frames, WIN - 1), next_frames, preferred_element_type=F32
    )
    pooled = (window_sums * (1.0 / WIN)).astype(BF)
    embedded = jnp.dot(pooled, embed_weight, preferred_element_type=F32) + embed_bias
    squares = jnp.sum(embedded * embedded, axis=1, keepdims=True)
    unit_rows = (embedded * lax.rsqrt(squares + epsilon)).astype(BF)

    near = neighbours // tile
    place = neighbours - near * tile
    is_tile = near[:, None, :] == jnp.arange(kept, dtype=jnp.int32)[None, :, None]
    marks = jnp.where(is_tile, place[:, None, :] + 1, 0)
    even = jnp.sum(marks[0::2], axis=0) - 1
    odd = jnp.sum(marks[1::2], axis=0) - 1
    seeds = initial_codes.astype(F32)
    seed_top, seed_rest = split2(seeds)
    extra = jnp.concatenate(
        [
            jnp.concatenate([even.astype(BF), odd.astype(BF)], axis=0),
            jnp.concatenate([seed_top, seed_rest], axis=0),
        ],
        axis=1,
    )
    got, owners = gather_stages(jnp.concatenate([unit_rows, extra], axis=0), shards)
    per = own_rows // tile
    col_tile = jnp.repeat(
        (owners[:, None] * per + jnp.arange(per, dtype=jnp.int32)[None, :]).reshape(-1), tile
    ).reshape(1, length)
    body = functools.partial(dense_kernel, tile, shards, own_rows, width, kept, vec_count)
    return pl.pallas_call(
        body,
        out_shape=(
            jax.ShapeDtypeStruct((kept, own_rows), F32),
            jax.ShapeDtypeStruct((vec_count, own_rows), F32),
        ),
        in_specs=[pl.BlockSpec(memory_space=pltpu.VMEM)] * 3,
        out_specs=(pl.BlockSpec(memory_space=pltpu.VMEM),) * 2,
        scratch_shapes=[
            pltpu.VMEM((length, width), BF),
            pltpu.VMEM((4 * kept, length), F32),
            pltpu.VMEM((4 * kept, length), F32),
            pltpu.VMEM((length, length), BF),
            pltpu.VMEM((length, length), BF),
            pltpu.VMEM((vec_count, length), F32),
        ],
        compiler_params=pltpu.CompilerParams(vmem_limit_bytes=56 * 1024 * 1024),
    )(col_tile, near, got)


def on_device(frames, offsets, neighbours, initial_codes, embed_weight, embed_bias):
    kept, own_rows = neighbours.shape
    shards = lax.axis_size("rows")
    length = own_rows * shards
    fits = (
        4 * length * length <= DENSE_BYTES
        and shards % 4 == 0
        and kept % 2 == 0
        and length % kept == 0
        and own_rows % (length // kept) == 0
        and length // kept <= 256
        and initial_codes.shape[0] == kept
        and embed_weight.shape[1] == 2 * own_rows
        and length % 512 == 0
    )
    chosen = on_device_dense if fits else on_device_sharded
    return chosen(frames, offsets, neighbours, initial_codes, embed_weight, embed_bias)


def solution(mesh):
    placed = (
        P(("groups", "rows"), None),
        P(("groups", "rows")),
        P(None, ("groups", "rows")),
        P(None, ("groups", "rows")),
        P(),
        P(),
    )
    return jax.shard_map(
        on_device,
        mesh=mesh,
        in_specs=placed,
        out_specs=(P(None, ("groups", "rows")), P(None, ("groups", "rows"))),
        check_vma=False,
    )
```

```python
import functools
import math

import jax
import jax.numpy as jnp
from jax import lax
from jax.experimental import pallas as pl
from jax.experimental.pallas import tpu as pltpu
from jax.sharding import PartitionSpec as P

WIN = 19
ITERS = 3


epsilon = 1e-06
sharpness = 8.0
seed_scale = 2.0 ** (-20)


def from_behind(block, axis, distance):
    devices = range(lax.axis_size(axis))
    route = [(i - distance, i) for i in devices if i - distance in devices]
    return lax.ppermute(block, axis, route)


def block_width(length, shard_rows):
    shards = length // shard_rows
    chosen = 1
    for factor in range(1, shards + 1):
        if shards % factor == 0 and factor * shard_rows <= 4096:
            chosen = factor
    return chosen * shard_rows


def on_device_sharded(frames, offsets, neighbours, initial_codes, embed_weight, embed_bias):
    own_rows = offsets.shape[0]
    own_frames = frames.shape[0]
    kept = neighbours.shape[0]
    my_index = lax.axis_index("rows")
    next_frames = from_behind(frames[: WIN - 1], "rows", -1)
    extended = jnp.concatenate([frames, next_frames], axis=0)
    window_start = offsets - my_index * own_frames
    positions = jnp.arange(extended.shape[0], dtype=jnp.int32)[None, :]
    begins = window_start[:, None]
    window_mask = ((positions >= begins) & (positions < begins + WIN)).astype(jnp.bfloat16)
    window_sums = jnp.dot(window_mask, extended, preferred_element_type=jnp.float32)
    pooled = (window_sums * (1.0 / WIN)).astype(jnp.bfloat16)
    embedded = jnp.dot(pooled, embed_weight, preferred_element_type=jnp.float32) + embed_bias
    squares = jnp.sum(embedded * embedded, axis=1, keepdims=True)
    unit_rows = (embedded * lax.rsqrt(squares + epsilon)).astype(jnp.bfloat16)
    portion = lax.all_gather(unit_rows, "rows", axis=0, tiled=True)
    length = portion.shape[0]
    block_cols = block_width(length, own_rows)

    def one_block(block_index, carried):
        first_col = block_index * block_cols
        candidates = lax.dynamic_slice_in_dim(portion, first_col, block_cols, 0)
        scores = lax.dot_general(
            unit_rows, candidates, (((1,), (1,)), ((), ())), preferred_element_type=jnp.float32
        )
        relative = neighbours - first_col
        inside = (relative >= 0) & (relative < block_cols)
        picked = jnp.take_along_axis(scores, jnp.clip(relative, 0, block_cols - 1).T, axis=1).T
        return carried + jnp.where(inside, picked, 0.0)

    cosine = lax.fori_loop(
        0, length // block_cols, one_block, jnp.zeros((kept, own_rows), jnp.float32)
    )
    affinity = jnp.exp(sharpness * (cosine - 1.0))
    vectors = initial_codes.astype(jnp.float32) * seed_scale
    vec_count = vectors.shape[0]
    carried = vectors
    for turn_index in range(ITERS):
        gathered = lax.all_gather(carried, "rows", axis=1, tiled=True)
        if turn_index > 0:
            gram_matrix = jnp.dot(gathered, gathered.T, precision=lax.Precision.HIGHEST)
            cholesky_factor = jnp.linalg.cholesky(gram_matrix)
            gathered = jax.scipy.linalg.solve_triangular(cholesky_factor, gathered, lower=True)
        current = lax.dynamic_slice_in_dim(gathered, my_index * own_rows, own_rows, 1)
        forward = jnp.sum(affinity[None] * jnp.take(gathered, neighbours, axis=1), axis=1)
        spread = (
            jnp.zeros((vec_count, gathered.shape[1]), jnp.float32)
            .at[:, neighbours.reshape(-1)]
            .add((affinity[None] * current[:, None, :]).reshape(vec_count, -1))
        )
        mixed = 0.5 * (forward + lax.psum_scatter(spread, "rows", scatter_dimension=1, tiled=True))
        carried = mixed
    partial_gram = jnp.dot(carried, carried.T, precision=lax.Precision.HIGHEST)
    gram_matrix = lax.psum(partial_gram, "rows")
    cholesky_factor = jnp.linalg.cholesky(gram_matrix)
    carried = jax.scipy.linalg.solve_triangular(cholesky_factor, carried, lower=True)
    return (affinity, carried)


BF = jnp.bfloat16
F32 = jnp.float32
DENSE_BYTES = 32 * 1024 * 1024
NT = (((1,), (1,)), ((), ()))


def split2(x):
    high = x.astype(BF)
    return high, (x - high.astype(F32)).astype(BF)


FLIPS = (0, 2, 1, 3)


def gather_stages(own, count):
    hop = lambda block, route: lax.ppermute(block, "rows", route)
    along = [own]
    for step in range(1, count // 4):
        along.append(hop(own, [(i, (i + 4 * step) % count) for i in range(count)]))
    line = jnp.stack(along)
    beside = hop(line, [(i, i ^ 2) for i in range(count)])
    core = [(i, i ^ 1) for i in range(count)]
    return line, beside, hop(line, core), hop(beside, core)


def orthonormal_factor(gram):
    size = gram.shape[0]
    lanes = 128 * (-(-2 * size // 128))
    panel = 8
    rows = lax.broadcasted_iota(jnp.int32, (size, size), 0)
    cols = lax.broadcasted_iota(jnp.int32, (size, size), 1)
    parts = [gram, (rows == cols).astype(F32)]
    if lanes > 2 * size:
        parts.append(jnp.zeros((size, lanes - 2 * size), F32))
    work = jnp.concatenate(parts, axis=1)
    row_ids = lax.broadcasted_iota(jnp.int32, (size, lanes), 0)
    for first in range(0, size, panel):
        wide = [
            jnp.broadcast_to(work[:, k : k + 1], (size, lanes))
            for k in range(first, first + panel)
        ]
        for m in range(panel):
            k = first + m
            inverse = 1.0 / wide[m][k : k + 1, :]
            factor = jnp.where(row_ids > k, wide[m] * inverse, 0.0)
            for later in range(m + 1, panel):
                wide[later] = wide[later] - factor * wide[later][k : k + 1, :]
            work = work - factor * work[k : k + 1, :]
    pivots = jnp.sum(jnp.where(rows == cols, work[:, :size], 0.0), axis=1, keepdims=True)
    return work[:, size : 2 * size] * lax.rsqrt(pivots)


def dense_kernel(tile, shards, own_rows, width, kept, vec_count, me_ref, near_ref, line_ref,
                 beside_ref, across_ref, corner_ref, aff_ref, vec_ref, unit, codes, spots, high,
                 start, spots_b, codes_b):
    length = shards * own_rows
    half = kept
    runs = (line_ref, beside_ref, across_ref, corner_ref)
    far = shards // 4
    lane = lax.broadcasted_iota(jnp.int32, (1, own_rows), 1)
    rank = lax.broadcasted_iota(jnp.int32, (half, own_rows), 0)
    inner = lax.rem(lane, tile).astype(F32)
    for s in range(shards):
        span = pl.ds(s * own_rows, own_rows)
        got_ref = runs[s // far]
        owner = lax.bitwise_xor(lax.rem(me_ref[0] + shards - 4 * (s % far), shards), FLIPS[s // far])
        member = (rank == owner * (own_rows // tile) + lane // tile).astype(F32)
        spots[pl.ds(0, half), span] = -inner * member
        spots[pl.ds(half, half), span] = -inner * member
        spots[pl.ds(2 * half, half), span] = 256.0 * member
        spots[pl.ds(3 * half, half), span] = member
        unit[span, :] = got_ref[s % far, :own_rows, :]
        extra = got_ref[s % far, own_rows:, :].astype(F32)
        even = extra[:half, :own_rows]
        odd = extra[half : 2 * half, :own_rows]
        product = even * odd
        upper = jnp.floor(product * (1.0 / 256.0))
        codes[pl.ds(0, half), span] = even
        codes[pl.ds(half, half), span] = odd
        codes[pl.ds(2 * half, half), span] = upper
        codes[pl.ds(3 * half, half), span] = product - 256.0 * upper
        start[:, span] = (
            extra[:vec_count, own_rows:] + extra[vec_count : 2 * vec_count, own_rows:]
        )
    col = lax.broadcasted_iota(jnp.int32, (1, length), 1)
    place = lax.rem(col, tile).astype(F32)

    gain = sharpness / math.log(2.0)
    chunk = 256
    tall = 512
    spots_b[...] = spots[...].astype(BF)
    codes_b[...] = codes[...].astype(BF)

    @pl.loop(0, length // tall)
    def _(b):
        span = pl.ds(pl.multiple_of(b * tall, tall), tall)
        my_unit = unit[span, :]
        my_codes = codes[:, span].T.astype(BF)
        my_spots = spots[:, span].T.astype(BF)
        my_place = lax.rem(lax.broadcasted_iota(jnp.int32, (tall, 1), 0), tile).astype(F32)
        for c in range(length // chunk):
            cols = pl.ds(c * chunk, chunk)
            scores = lax.dot_general(my_unit, unit[cols, :], NT, preferred_element_type=F32)
            ahead = jnp.dot(my_codes, spots_b[:, cols], preferred_element_type=F32)
            behind = jnp.dot(my_spots, codes_b[:, cols], preferred_element_type=F32)
            here = place[:, c * chunk : (c + 1) * chunk]
            share = jnp.where(ahead == -here * here, 0.5, 0.0) + jnp.where(
                behind == -my_place * my_place, 0.5, 0.0
            )
            weight = jnp.exp2(scores * gain - gain) * share
            high[span, cols] = weight.astype(BF)

    own = pl.ds(0, own_rows)
    spread = spots_b[pl.ds(3 * half, half), :]
    scores = lax.dot_general(unit[own, :], unit[...], NT, preferred_element_type=F32)
    weight = jnp.exp2(scores * gain - gain)
    found = []
    for parity in range(2):
        code = codes[pl.ds(parity * half, half), own].T.astype(BF)
        mask = jnp.dot(code, spread, preferred_element_type=F32) == place
        value = jnp.where(mask, weight, 0.0)
        top, rest = split2(value)
        found.append(
            lax.dot_general(spread, top, NT, preferred_element_type=F32)
            + lax.dot_general(spread, rest, NT, preferred_element_type=F32)
        )
    near = near_ref[...]
    odd_row = lax.rem(lax.broadcasted_iota(jnp.int32, near.shape, 0), 2) == 1
    result = jnp.zeros(near.shape, F32)
    for t in range(half):
        pick = jnp.where(odd_row, found[1][t : t + 1, :], found[0][t : t + 1, :])
        result = result + jnp.where(near == t, pick, 0.0)
    aff_ref[...] = result

    current = start[...] * seed_scale
    for turn in range(ITERS):
        top, rest = split2(current)
        both = jnp.concatenate([top, rest], axis=0)
        first = jnp.dot(both, high[...], preferred_element_type=F32)
        mixed = first[:vec_count] + first[vec_count:]
        gram = lax.dot_general(
            mixed, mixed, NT, preferred_element_type=F32, precision=lax.Precision.HIGHEST
        )
        factor = orthonormal_factor(gram)
        if turn == ITERS - 1:
            mixed = mixed[:, :own_rows]
        current = jnp.dot(
            factor, mixed, preferred_element_type=F32, precision=lax.Precision.HIGHEST
        )
    vec_ref[...] = current


def on_device_dense(frames, offsets, neighbours, initial_codes, embed_weight, embed_bias):
    own_rows = offsets.shape[0]
    own_frames = frames.shape[0]
    kept = neighbours.shape[0]
    vec_count = initial_codes.shape[0]
    shards = lax.axis_size("rows")
    length = own_rows * shards
    tile = length // kept
    width = embed_weight.shape[1]
    my_index = lax.axis_index("rows")
    next_frames = from_behind(frames[: WIN - 1], "rows", -1)
    begins = (offsets - my_index * own_frames)[:, None]

    def window_mask(first, count):
        positions = first + jnp.arange(count, dtype=jnp.int32)[None, :]
        return ((positions >= begins) & (positions < begins + WIN)).astype(BF)

    window_sums = jnp.dot(
        window_mask(0, own_frames), frames, preferred_element_type=F32
    ) + jnp.dot(
        window_mask(own_frames, WIN - 1), next_frames, preferred_element_type=F32
    )
    pooled = (window_sums * (1.0 / WIN)).astype(BF)
    embedded = jnp.dot(pooled, embed_weight, preferred_element_type=F32) + embed_bias
    squares = jnp.sum(embedded * embedded, axis=1, keepdims=True)
    unit_rows = (embedded * lax.rsqrt(squares + epsilon)).astype(BF)

    near = neighbours // tile
    place = neighbours - near * tile
    is_tile = near[:, None, :] == jnp.arange(kept, dtype=jnp.int32)[None, :, None]
    marks = jnp.where(is_tile, place[:, None, :] + 1, 0)
    even = jnp.sum(marks[0::2], axis=0) - 1
    odd = jnp.sum(marks[1::2], axis=0) - 1
    seeds = initial_codes.astype(F32)
    seed_top, seed_rest = split2(seeds)
    extra = jnp.concatenate(
        [
            jnp.concatenate([even.astype(BF), odd.astype(BF)], axis=0),
            jnp.concatenate([seed_top, seed_rest], axis=0),
        ],
        axis=1,
    )
    runs = gather_stages(jnp.concatenate([unit_rows, extra], axis=0), shards)
    body = functools.partial(dense_kernel, tile, shards, own_rows, width, kept, vec_count)
    return pl.pallas_call(
        body,
        out_shape=(
            jax.ShapeDtypeStruct((kept, own_rows), F32),
            jax.ShapeDtypeStruct((vec_count, own_rows), F32),
        ),
        in_specs=[pl.BlockSpec(memory_space=pltpu.SMEM)]
        + [pl.BlockSpec(memory_space=pltpu.VMEM)] * 5,
        out_specs=(pl.BlockSpec(memory_space=pltpu.VMEM),) * 2,
        scratch_shapes=[
            pltpu.VMEM((length, width), BF),
            pltpu.VMEM((4 * kept, length), F32),
            pltpu.VMEM((4 * kept, length), F32),
            pltpu.VMEM((length, length), BF),
            pltpu.VMEM((vec_count, length), F32),
            pltpu.VMEM((4 * kept, length), BF),
            pltpu.VMEM((4 * kept, length), BF),
        ],
        compiler_params=pltpu.CompilerParams(vmem_limit_bytes=56 * 1024 * 1024),
    )(my_index.reshape(1).astype(jnp.int32), near, *runs)


def on_device(frames, offsets, neighbours, initial_codes, embed_weight, embed_bias):
    kept, own_rows = neighbours.shape
    shards = lax.axis_size("rows")
    length = own_rows * shards
    fits = (
        4 * length * length <= DENSE_BYTES
        and shards % 4 == 0
        and kept % 2 == 0
        and length % kept == 0
        and own_rows % (length // kept) == 0
        and length // kept <= 256
        and initial_codes.shape[0] == kept
        and embed_weight.shape[1] == 2 * own_rows
        and length % 1024 == 0
    )
    chosen = on_device_dense if fits else on_device_sharded
    return chosen(frames, offsets, neighbours, initial_codes, embed_weight, embed_bias)


def solution(mesh):
    placed = (
        P(("groups", "rows"), None),
        P(("groups", "rows")),
        P(None, ("groups", "rows")),
        P(None, ("groups", "rows")),
        P(),
        P(),
    )
    return jax.shard_map(
        on_device,
        mesh=mesh,
        in_specs=placed,
        out_specs=(P(None, ("groups", "rows")), P(None, ("groups", "rows"))),
        check_vma=False,
    )
```

```python
import functools
import math

import jax
import jax.numpy as jnp
from jax import lax
from jax.experimental import pallas as pl
from jax.experimental.pallas import tpu as pltpu
from jax.sharding import PartitionSpec as P

WIN = 19
ITERS = 3


epsilon = 1e-06
sharpness = 8.0
seed_scale = 2.0 ** (-20)


def from_behind(block, axis, distance):
    devices = range(lax.axis_size(axis))
    route = [(i - distance, i) for i in devices if i - distance in devices]
    return lax.ppermute(block, axis, route)


def block_width(length, shard_rows):
    shards = length // shard_rows
    chosen = 1
    for factor in range(1, shards + 1):
        if shards % factor == 0 and factor * shard_rows <= 4096:
            chosen = factor
    return chosen * shard_rows


def on_device_sharded(frames, offsets, neighbours, initial_codes, embed_weight, embed_bias):
    own_rows = offsets.shape[0]
    own_frames = frames.shape[0]
    kept = neighbours.shape[0]
    my_index = lax.axis_index("rows")
    next_frames = from_behind(frames[: WIN - 1], "rows", -1)
    extended = jnp.concatenate([frames, next_frames], axis=0)
    window_start = offsets - my_index * own_frames
    positions = jnp.arange(extended.shape[0], dtype=jnp.int32)[None, :]
    begins = window_start[:, None]
    window_mask = ((positions >= begins) & (positions < begins + WIN)).astype(jnp.bfloat16)
    window_sums = jnp.dot(window_mask, extended, preferred_element_type=jnp.float32)
    pooled = (window_sums * (1.0 / WIN)).astype(jnp.bfloat16)
    embedded = jnp.dot(pooled, embed_weight, preferred_element_type=jnp.float32) + embed_bias
    squares = jnp.sum(embedded * embedded, axis=1, keepdims=True)
    unit_rows = (embedded * lax.rsqrt(squares + epsilon)).astype(jnp.bfloat16)
    portion = lax.all_gather(unit_rows, "rows", axis=0, tiled=True)
    length = portion.shape[0]
    block_cols = block_width(length, own_rows)

    def one_block(block_index, carried):
        first_col = block_index * block_cols
        candidates = lax.dynamic_slice_in_dim(portion, first_col, block_cols, 0)
        scores = lax.dot_general(
            unit_rows, candidates, (((1,), (1,)), ((), ())), preferred_element_type=jnp.float32
        )
        relative = neighbours - first_col
        inside = (relative >= 0) & (relative < block_cols)
        picked = jnp.take_along_axis(scores, jnp.clip(relative, 0, block_cols - 1).T, axis=1).T
        return carried + jnp.where(inside, picked, 0.0)

    cosine = lax.fori_loop(
        0, length // block_cols, one_block, jnp.zeros((kept, own_rows), jnp.float32)
    )
    affinity = jnp.exp(sharpness * (cosine - 1.0))
    vectors = initial_codes.astype(jnp.float32) * seed_scale
    vec_count = vectors.shape[0]
    carried = vectors
    for turn_index in range(ITERS):
        gathered = lax.all_gather(carried, "rows", axis=1, tiled=True)
        if turn_index > 0:
            gram_matrix = jnp.dot(gathered, gathered.T, precision=lax.Precision.HIGHEST)
            cholesky_factor = jnp.linalg.cholesky(gram_matrix)
            gathered = jax.scipy.linalg.solve_triangular(cholesky_factor, gathered, lower=True)
        current = lax.dynamic_slice_in_dim(gathered, my_index * own_rows, own_rows, 1)
        forward = jnp.sum(affinity[None] * jnp.take(gathered, neighbours, axis=1), axis=1)
        spread = (
            jnp.zeros((vec_count, gathered.shape[1]), jnp.float32)
            .at[:, neighbours.reshape(-1)]
            .add((affinity[None] * current[:, None, :]).reshape(vec_count, -1))
        )
        mixed = 0.5 * (forward + lax.psum_scatter(spread, "rows", scatter_dimension=1, tiled=True))
        carried = mixed
    partial_gram = jnp.dot(carried, carried.T, precision=lax.Precision.HIGHEST)
    gram_matrix = lax.psum(partial_gram, "rows")
    cholesky_factor = jnp.linalg.cholesky(gram_matrix)
    carried = jax.scipy.linalg.solve_triangular(cholesky_factor, carried, lower=True)
    return (affinity, carried)


BF = jnp.bfloat16
F32 = jnp.float32
DENSE_BYTES = 32 * 1024 * 1024
NT = (((1,), (1,)), ((), ()))


def split2(x):
    high = x.astype(BF)
    return high, (x - high.astype(F32)).astype(BF)


FLIPS = (0, 2, 1, 3)


def gather_stages(own, count):
    hop = lambda block, route: lax.ppermute(block, "rows", route)
    beside = [(i, i ^ 2) for i in range(count)]
    across = [(i, i ^ 1) for i in range(count)]
    along = [
        hop(own, [(i, (i + 4 * step) % count) for i in range(count)])
        for step in range(1, count // 4)
    ]
    *along, own_beside = lax.optimization_barrier((*along, hop(own, beside)))
    others = jnp.stack(along)
    others_beside = hop(others, beside)
    moved = [hop(block, across) for block in (own, others, own_beside)]
    others_beside, *moved = lax.optimization_barrier((others_beside, *moved))
    return own, others, own_beside, others_beside, *moved, hop(others_beside, across)


def orthonormal_factor(gram):
    size = gram.shape[0]
    lanes = 128 * (-(-2 * size // 128))
    panel = 8
    rows = lax.broadcasted_iota(jnp.int32, (size, size), 0)
    cols = lax.broadcasted_iota(jnp.int32, (size, size), 1)
    parts = [gram, (rows == cols).astype(F32)]
    if lanes > 2 * size:
        parts.append(jnp.zeros((size, lanes - 2 * size), F32))
    work = jnp.concatenate(parts, axis=1)
    row_ids = lax.broadcasted_iota(jnp.int32, (size, lanes), 0)
    for first in range(0, size, panel):
        wide = [
            jnp.broadcast_to(work[:, k : k + 1], (size, lanes))
            for k in range(first, first + panel)
        ]
        for m in range(panel):
            k = first + m
            inverse = 1.0 / wide[m][k : k + 1, :]
            factor = jnp.where(row_ids > k, wide[m] * inverse, 0.0)
            for later in range(m + 1, panel):
                wide[later] = wide[later] - factor * wide[later][k : k + 1, :]
            work = work - factor * work[k : k + 1, :]
    pivots = jnp.sum(jnp.where(rows == cols, work[:, :size], 0.0), axis=1, keepdims=True)
    return work[:, size : 2 * size] * lax.rsqrt(pivots)


def dense_kernel(tile, shards, own_rows, width, kept, vec_count, me_ref, near_ref,
                 own_ref, own_line_ref, beside_ref, beside_line_ref,
                 across_ref, across_line_ref, corner_ref, corner_line_ref, aff_ref, vec_ref, unit, codes, spots, high,
                 start, spots_b, codes_b):
    length = shards * own_rows
    half = kept
    firsts = (own_ref, beside_ref, across_ref, corner_ref)
    lines = (own_line_ref, beside_line_ref, across_line_ref, corner_line_ref)
    far = shards // 4
    lane = lax.broadcasted_iota(jnp.int32, (1, own_rows), 1)
    rank = lax.broadcasted_iota(jnp.int32, (half, own_rows), 0)
    inner = lax.rem(lane, tile).astype(F32)
    for s in range(shards):
        span = pl.ds(s * own_rows, own_rows)
        got_ref = lines[s // far].at[s % far - 1] if s % far else firsts[s // far]
        owner = lax.bitwise_xor(lax.rem(me_ref[0] + shards - 4 * (s % far), shards), FLIPS[s // far])
        member = (rank == owner * (own_rows // tile) + lane // tile).astype(F32)
        spots[pl.ds(0, half), span] = -inner * member
        spots[pl.ds(half, half), span] = -inner * member
        spots[pl.ds(2 * half, half), span] = 256.0 * member
        spots[pl.ds(3 * half, half), span] = member
        unit[span, :] = got_ref[:own_rows, :]
        extra = got_ref[own_rows:, :].astype(F32)
        even = extra[:half, :own_rows]
        odd = extra[half : 2 * half, :own_rows]
        product = even * odd
        upper = jnp.floor(product * (1.0 / 256.0))
        codes[pl.ds(0, half), span] = even
        codes[pl.ds(half, half), span] = odd
        codes[pl.ds(2 * half, half), span] = upper
        codes[pl.ds(3 * half, half), span] = product - 256.0 * upper
        start[:, span] = (
            extra[:vec_count, own_rows:] + extra[vec_count : 2 * vec_count, own_rows:]
        )
    col = lax.broadcasted_iota(jnp.int32, (1, length), 1)
    place = lax.rem(col, tile).astype(F32)

    gain = sharpness / math.log(2.0)
    chunk = 256
    tall = 512
    spots_b[...] = spots[...].astype(BF)
    codes_b[...] = codes[...].astype(BF)

    @pl.loop(0, length // tall)
    def _(b):
        span = pl.ds(pl.multiple_of(b * tall, tall), tall)
        my_unit = unit[span, :]
        my_codes = codes[:, span].T.astype(BF)
        my_spots = spots[:, span].T.astype(BF)
        my_place = lax.rem(lax.broadcasted_iota(jnp.int32, (tall, 1), 0), tile).astype(F32)
        for c in range(length // chunk):
            cols = pl.ds(c * chunk, chunk)
            scores = lax.dot_general(my_unit, unit[cols, :], NT, preferred_element_type=F32)
            ahead = jnp.dot(my_codes, spots_b[:, cols], preferred_element_type=F32)
            behind = jnp.dot(my_spots, codes_b[:, cols], preferred_element_type=F32)
            here = place[:, c * chunk : (c + 1) * chunk]
            share = jnp.where(ahead == -here * here, 0.5, 0.0) + jnp.where(
                behind == -my_place * my_place, 0.5, 0.0
            )
            weight = jnp.exp2(scores * gain - gain) * share
            high[span, cols] = weight.astype(BF)

    own = pl.ds(0, own_rows)
    spread = spots_b[pl.ds(3 * half, half), :]
    scores = lax.dot_general(unit[own, :], unit[...], NT, preferred_element_type=F32)
    weight = jnp.exp2(scores * gain - gain)
    found = []
    for parity in range(2):
        code = codes[pl.ds(parity * half, half), own].T.astype(BF)
        mask = jnp.dot(code, spread, preferred_element_type=F32) == place
        value = jnp.where(mask, weight, 0.0)
        top, rest = split2(value)
        found.append(
            lax.dot_general(spread, top, NT, preferred_element_type=F32)
            + lax.dot_general(spread, rest, NT, preferred_element_type=F32)
        )
    near = near_ref[...]
    odd_row = lax.rem(lax.broadcasted_iota(jnp.int32, near.shape, 0), 2) == 1
    result = jnp.zeros(near.shape, F32)
    for t in range(half):
        pick = jnp.where(odd_row, found[1][t : t + 1, :], found[0][t : t + 1, :])
        result = result + jnp.where(near == t, pick, 0.0)
    aff_ref[...] = result

    current = start[...] * seed_scale
    for turn in range(ITERS):
        top, rest = split2(current)
        both = jnp.concatenate([top, rest], axis=0)
        first = jnp.dot(both, high[...], preferred_element_type=F32)
        mixed = first[:vec_count] + first[vec_count:]
        gram = lax.dot_general(
            mixed, mixed, NT, preferred_element_type=F32, precision=lax.Precision.HIGHEST
        )
        factor = orthonormal_factor(gram)
        if turn == ITERS - 1:
            mixed = mixed[:, :own_rows]
        current = jnp.dot(
            factor, mixed, preferred_element_type=F32, precision=lax.Precision.HIGHEST
        )
    vec_ref[...] = current


def on_device_dense(frames, offsets, neighbours, initial_codes, embed_weight, embed_bias):
    own_rows = offsets.shape[0]
    own_frames = frames.shape[0]
    kept = neighbours.shape[0]
    vec_count = initial_codes.shape[0]
    shards = lax.axis_size("rows")
    length = own_rows * shards
    tile = length // kept
    width = embed_weight.shape[1]
    my_index = lax.axis_index("rows")
    next_frames = from_behind(frames[: WIN - 1], "rows", -1)
    begins = (offsets - my_index * own_frames)[:, None]

    def window_mask(first, count):
        positions = first + jnp.arange(count, dtype=jnp.int32)[None, :]
        return ((positions >= begins) & (positions < begins + WIN)).astype(BF)

    window_sums = jnp.dot(
        window_mask(0, own_frames), frames, preferred_element_type=F32
    ) + jnp.dot(
        window_mask(own_frames, WIN - 1), next_frames, preferred_element_type=F32
    )
    pooled = (window_sums * (1.0 / WIN)).astype(BF)
    embedded = jnp.dot(pooled, embed_weight, preferred_element_type=F32) + embed_bias
    squares = jnp.sum(embedded * embedded, axis=1, keepdims=True)
    unit_rows = (embedded * lax.rsqrt(squares + epsilon)).astype(BF)

    near = neighbours // tile
    place = neighbours - near * tile
    is_tile = near[:, None, :] == jnp.arange(kept, dtype=jnp.int32)[None, :, None]
    marks = jnp.where(is_tile, place[:, None, :] + 1, 0)
    even = jnp.sum(marks[0::2], axis=0) - 1
    odd = jnp.sum(marks[1::2], axis=0) - 1
    seeds = initial_codes.astype(F32)
    seed_top, seed_rest = split2(seeds)
    extra = jnp.concatenate(
        [
            jnp.concatenate([even.astype(BF), odd.astype(BF)], axis=0),
            jnp.concatenate([seed_top, seed_rest], axis=0),
        ],
        axis=1,
    )
    runs = gather_stages(jnp.concatenate([unit_rows, extra], axis=0), shards)
    body = functools.partial(dense_kernel, tile, shards, own_rows, width, kept, vec_count)
    return pl.pallas_call(
        body,
        out_shape=(
            jax.ShapeDtypeStruct((kept, own_rows), F32),
            jax.ShapeDtypeStruct((vec_count, own_rows), F32),
        ),
        in_specs=[pl.BlockSpec(memory_space=pltpu.SMEM)]
        + [pl.BlockSpec(memory_space=pltpu.VMEM)] * 9,
        out_specs=(pl.BlockSpec(memory_space=pltpu.VMEM),) * 2,
        scratch_shapes=[
            pltpu.VMEM((length, width), BF),
            pltpu.VMEM((4 * kept, length), F32),
            pltpu.VMEM((4 * kept, length), F32),
            pltpu.VMEM((length, length), BF),
            pltpu.VMEM((vec_count, length), F32),
            pltpu.VMEM((4 * kept, length), BF),
            pltpu.VMEM((4 * kept, length), BF),
        ],
        compiler_params=pltpu.CompilerParams(vmem_limit_bytes=56 * 1024 * 1024),
    )(my_index.reshape(1).astype(jnp.int32), near, *runs)


def on_device(frames, offsets, neighbours, initial_codes, embed_weight, embed_bias):
    kept, own_rows = neighbours.shape
    shards = lax.axis_size("rows")
    length = own_rows * shards
    fits = (
        4 * length * length <= DENSE_BYTES
        and shards % 4 == 0
        and shards > 4
        and kept % 2 == 0
        and length % kept == 0
        and own_rows % (length // kept) == 0
        and length // kept <= 256
        and initial_codes.shape[0] == kept
        and embed_weight.shape[1] == 2 * own_rows
        and length % 1024 == 0
    )
    chosen = on_device_dense if fits else on_device_sharded
    return chosen(frames, offsets, neighbours, initial_codes, embed_weight, embed_bias)


def solution(mesh):
    placed = (
        P(("groups", "rows"), None),
        P(("groups", "rows")),
        P(None, ("groups", "rows")),
        P(None, ("groups", "rows")),
        P(),
        P(),
    )
    return jax.shard_map(
        on_device,
        mesh=mesh,
        in_specs=placed,
        out_specs=(P(None, ("groups", "rows")), P(None, ("groups", "rows"))),
        check_vma=False,
    )
```
